32 devices in a mesh: row: 4 (over z), col: 8 (over y, x, core).
Axes of the slice: x: 2, y: 2, z: 4, core: 2. Of those that a mesh axis runs over, the one named last changes fastest.
Arguments:
- factor_wide: float32 [4, 4, 2, 8, 512, 512], P(None, 'row', None, 'col'), may hold values from -1 to 2, as said below
- factor_narrow: bfloat16 [4, 4, 2, 8, 512, 512], P(None, 'row', None, 'col'), may hold values from -1 to 2, as said below
- flags: int32 [4, 4, 2, 8], P(None, 'row', None, 'col'), may hold values from 0 to 1
- forward_solution: float32 [2, 8, 512, 128], P(None, 'col'), may hold values from -0.5 to 0.5
- solution_grad: float32 [2, 8, 512, 128], P(None, 'col'), may hold values from -1.8 to 1.8
Outputs:
- rhs_grad: float32 [4, 4, 512, 128], P(None, 'row')
- factor_grad: float32 [4, 4, 2, 8, 512, 512], P(None, 'row', None, 'col')
The draws below stay inside these ranges and needn't reach their ends.
Inputs may be any that keep to these rules, and one draw needn't show every extreme that they name: `factor_wide`: the diagonal entries of every diagonal tile lie between 1 and 2. `factor_narrow`: the diagonal entries of every diagonal tile lie between 1 and 2.
All inputs are finite; a program needn't handle non-finite values.
Results may differ from the reference program's by a relative error of at most 0.0003.
Values sent between devices are 32-bit elements; how exact they have to be, the bound alone decides.
A program may use at most 64 MiB of HBM per device.

```python
import math
import jax
import jax.numpy as jnp
from jax import lax

TB = 512
NT = 16
R = 128
N_ROW = 4
N_COL = 8


coupling = 3.0


def factor_law(key):
    shape = (NT // N_ROW, N_ROW, NT // N_COL, N_COL, TB, TB)
    spread = jax.random.normal(key, shape, jnp.float32)
    diagonal = jax.random.uniform(jax.random.fold_in(key, 5), shape, jnp.float32, 1.0, 2.0)
    scaled = spread * (coupling / math.sqrt(NT * TB))
    row_shape = (NT // N_ROW, N_ROW, 1, 1, 1, 1)
    col_shape = (1, 1, NT // N_COL, N_COL, 1, 1)
    inner_shape = (1, 1, 1, 1, TB, TB)
    tile_row = lax.broadcasted_iota(jnp.int32, row_shape, 0) * N_ROW + lax.broadcasted_iota(jnp.int32, row_shape, 1)
    tile_col = lax.broadcasted_iota(jnp.int32, col_shape, 2) * N_COL + lax.broadcasted_iota(jnp.int32, col_shape, 3)
    inner_row = lax.broadcasted_iota(jnp.int32, inner_shape, 4)
    inner_col = lax.broadcasted_iota(jnp.int32, inner_shape, 5)
    on_diagonal = (tile_row == tile_col) & (inner_row == inner_col)
    return jnp.where(on_diagonal, diagonal, scaled)


def draw_factor_wide(key, part):
    return factor_law(jax.random.fold_in(key, 11))


def draw_factor_narrow(key, part):
    return factor_law(jax.random.fold_in(key, 23)).astype(jnp.bfloat16)


def with_ends(entries, rng, smallest, high):
    longest = entries.shape.index(max(entries.shape))
    spots = []
    for shift in (0, 1):
        where = [jax.random.randint(jax.random.fold_in(rng, axis), (), 0, length) for axis, length in enumerate(entries.shape)]
        where[longest] = (where[longest] + shift) % entries.shape[longest]
        spots.append(tuple(where))
    return entries.at[spots[0]].set(smallest).at[spots[1]].set(high)


def block_scale(rng, shape, split, low, high):
    loudness = 1.0
    for position, shards_of in split:
        heights = jax.random.uniform(jax.random.fold_in(jax.random.fold_in(rng, 6), position), (shards_of,), jnp.float32, low / len(split), high / len(split))
        loudness = loudness * jnp.repeat(jnp.exp(heights), shape[position] // shards_of).reshape((-1,) + (1,) * (len(shape) - 1 - position))
    return loudness


def normal_values(stream_key, shape, width, most, cuts=(), held_as=jnp.bfloat16):
    drawn = jax.random.normal(stream_key, shape, jnp.float32) * width
    if len(cuts) > 0:
        drawn = block_scale(stream_key, shape, cuts, -0.22, 0.18) * drawn
    return jnp.clip(drawn, min=-most, max=most).astype(held_as)


def setup_inputs(seed: int = 0) -> dict:
    seeds = jax.random.split(jax.random.key(seed), 6)
    factor_wide = draw_factor_wide(jax.random.fold_in(seeds[5], 71), 0)
    factor_narrow = draw_factor_narrow(jax.random.fold_in(seeds[5], 71), 0)
    flags = with_ends(jax.random.randint(seeds[2], (NT // N_ROW, N_ROW, NT // N_COL, N_COL), 0, 2), jax.random.fold_in(seeds[2], 1), 0, 1).astype(jnp.int32)
    forward_solution = normal_values(seeds[3], (NT // N_COL, N_COL, TB, R), R ** -0.5, 0.5, ((1, 8),), jnp.float32)
    solution_grad = normal_values(seeds[4], (NT // N_COL, N_COL, TB, R), 0.3, 1.8, ((1, 8),), jnp.float32)
    return {"factor_wide": factor_wide, "factor_narrow": factor_narrow, "flags": flags, "forward_solution": forward_solution, "solution_grad": solution_grad}


HIGHEST_PRECISION = lax.Precision.HIGHEST

def lower_mask(row_index, col_index, tile_width):
    inner_mask = lax.broadcasted_iota(jnp.int32, (tile_width, tile_width), 0) >= lax.broadcasted_iota(jnp.int32, (tile_width, tile_width), 1)
    return (row_index > col_index) | (row_index == col_index) & inner_mask

def reference(factor_wide, factor_narrow, flags, forward_solution, solution_grad):
    chosen = jnp.where(flags[:, :, :, :, None, None] == 1, factor_narrow.astype(jnp.float32), factor_wide)
    factor_tiles = chosen.reshape(NT, NT, TB, TB)
    solution_tiles = forward_solution.reshape(NT, TB, R)
    target_tiles = solution_grad.reshape(NT, TB, R)
    solved_tiles = [None] * NT
    for target in range(NT - 1, -1, -1):
        right_side = target_tiles[target]
        for source in range(target + 1, NT):
            right_side = right_side - jnp.dot(factor_tiles[source, target].T.astype(jnp.float32), solved_tiles[source].astype(jnp.float32), precision=HIGHEST_PRECISION, preferred_element_type=jnp.float32)
        solved_tiles[target] = lax.linalg.triangular_solve(factor_tiles[target, target], right_side, left_side=True, lower=True, transpose_a=True)
    rhs_grad = jnp.stack(solved_tiles)
    products = -jnp.einsum('akr,blr->abkl', rhs_grad, solution_tiles, precision=HIGHEST_PRECISION)
    tile_index = jnp.arange(NT, dtype=jnp.int32)
    masks = lower_mask(tile_index[:, None, None, None], tile_index[None, :, None, None], TB)
    factor_grad = jnp.where(masks, products, jnp.zeros_like(products))
    return (rhs_grad.reshape(NT // N_ROW, N_ROW, TB, R), factor_grad.reshape(NT // N_ROW, N_ROW, NT // N_COL, N_COL, TB, TB))
```

```python
import functools

import jax
import jax.numpy as jnp
from jax import lax
from jax.experimental import pallas as pl
from jax.experimental.pallas import tpu as pltpu
from jax.sharding import PartitionSpec as P

BASE_BLOCK = 128
CHUNKS = 4
MESH = pl.DeviceIdType.MESH
VMEM_LIMIT = 60 * 1024 * 1024


def split(value):
    high = value.astype(jnp.bfloat16)
    return high, (value - high.astype(jnp.float32)).astype(jnp.bfloat16)


def split_product(value, high, low):
    count = value.shape[0]
    value_high, value_low = split(value)
    both = jnp.concatenate([value_high, value_low], axis=0)
    first = jnp.dot(both, high, preferred_element_type=jnp.float32)
    second = jnp.dot(value_high, low, preferred_element_type=jnp.float32)
    return first[:count] + (first[count:] + second)


def product(a, b):
    a_high, a_low = split(a)
    b_high, b_low = split(b)
    left = jnp.concatenate([a_high, a_low, a_high], axis=1)
    right = jnp.concatenate([b_high, b_high, b_low], axis=0)
    return jnp.dot(left, right, preferred_element_type=jnp.float32)


def invert(tile_ref, inverse_ref):
    width = tile_ref.shape[0]
    base = min(BASE_BLOCK, width)
    row = lax.broadcasted_iota(jnp.int32, (base, base), 0)
    col = lax.broadcasted_iota(jnp.int32, (base, base), 1)
    starts = range(0, width, base)
    blocks = [tile_ref[at:at + base, at:at + base] for at in starts]
    inverses = [jnp.where(row == col, 1.0 / jnp.where(row == col, b, 1.0), 0.0) for b in blocks]
    size = 1
    while size < base:
        corner = (row // (2 * size) == col // (2 * size)) & (row // size > col // size)
        halves = [product(x, jnp.where(corner, b, 0.0)) for x, b in zip(inverses, blocks)]
        inverses = [x - product(h, x) for x, h in zip(inverses, halves)]
        size *= 2
    inverse_ref[...] = jnp.zeros((width, width), jnp.float32)
    for at, x in zip(starts, inverses):
        inverse_ref[at:at + base, at:at + base] = x
    while size < width:
        for at in range(0, width, 2 * size):
            top, low = slice(at, at + size), slice(at + size, at + 2 * size)
            half = product(inverse_ref[low, low], tile_ref[low, top])
            inverse_ref[low, top] = -product(half, inverse_ref[top, top])
        size *= 2


def sweep_kernel(
    rows, cols, wide_ref, narrow_ref, flags_ref, target_ref, solved_ref,
    tiles, narrows, total, chain, parts, below, inverse, weights, pairs,
    load_sem, chain_send, chain_recv, plane_send, plane_recv,
    part_send, part_recv, below_send, below_recv,
):
    my_row, my_col = lax.axis_index("row"), lax.axis_index("col")
    local_rows, local_cols = tiles.shape[0], tiles.shape[1]
    rhs, width = total.shape[1], total.shape[2]
    chunk = rhs // CHUNKS
    count = local_rows * rows
    gaps = [d for d in range(2, rows + 2) if d != rows]
    urgent = [d for d in (2, 3) if d in gaps and d < cols]
    calm = [o for o in range(2, cols) if o not in urgent] + [1]

    def away(row_step, col_step):
        return (lax.rem(my_row + row_step + rows, rows), lax.rem(my_col + col_step + cols, cols))

    def target_of(s):
        return my_col + cols * s

    def owns(s):
        return lax.rem(target_of(s), rows) == my_row

    def loads(a, s):
        return (
            pltpu.make_async_copy(wide_ref.at[a, 0, s, 0], tiles.at[a, s], load_sem.at[a, s, 0]),
            pltpu.make_async_copy(narrow_ref.at[a, 0, s, 0], narrows.at[a, s], load_sem.at[a, s, 1]),
        )

    def start_loads(s):
        for a in reversed(range(local_rows)):
            @pl.when(a * rows + my_row >= target_of(s))
            def _():
                for copy in loads(a, s):
                    copy.start()

    def tile_value(a, s, at, size):
        flag = jnp.full((size, width), flags_ref[a, 0, s, 0], jnp.int32)
        narrow = narrows[a, s, pl.ds(at, size), :].astype(jnp.float32)
        return jnp.where(flag == 1, narrow, tiles[a, s, pl.ds(at, size), :])

    def settle(a, s, use):
        for copy in loads(a, s):
            copy.wait()
        size = min(128, width)

        def piece(p, carry):
            at = pl.multiple_of(p * size, size)
            use(at, size, tile_value(a, s, at, size))
            return carry

        lax.fori_loop(0, width // size, piece, 0)

    def settle_in_place(a, s):
        def use(at, size, value):
            tiles[a, s, pl.ds(at, size), :] = value
        settle(a, s, use)

    def settle_pair(a, s):
        def use(at, size, value):
            high, low = split(value)
            pairs[s, 0, pl.ds(at, size), :] = high
            pairs[s, 1, pl.ds(at, size), :] = low
        settle(a, s, use)

    def span(c):
        return pl.ds(pl.multiple_of(c * chunk, chunk), chunk)

    def chain_copy(slot, landing, c):
        return pltpu.make_async_remote_copy(
            src_ref=solved_ref.at[slot, span(c)], dst_ref=chain.at[landing, span(c)],
            send_sem=chain_send.at[slot, c], recv_sem=chain_recv.at[landing, c],
            device_id=away(-1, -1), device_id_type=MESH,
        )

    def plane_chunk(slot, offset, c):
        return pltpu.make_async_remote_copy(
            src_ref=solved_ref.at[slot, span(c)], dst_ref=solved_ref.at[slot, span(c)],
            send_sem=plane_send.at[slot, offset, c], recv_sem=plane_recv.at[slot, c],
            device_id=away(0, -offset), device_id_type=MESH,
        )

    def plane_whole(slot, offset):
        return pltpu.make_async_remote_copy(
            src_ref=solved_ref.at[slot], dst_ref=solved_ref.at[slot],
            send_sem=plane_send.at[slot, offset, 0], recv_sem=plane_recv.at[slot, 0],
            device_id=away(0, -offset), device_id_type=MESH,
        )

    def part_copy(slot, where, gap, c):
        return pltpu.make_async_remote_copy(
            src_ref=total.at[slot, span(c)], dst_ref=parts.at[slot, where, span(c)],
            send_sem=part_send.at[slot, c], recv_sem=part_recv.at[slot, where, c],
            device_id=away((-gap) % rows, 0), device_id_type=MESH,
        )

    def below_copy(a, s):
        return pltpu.make_async_remote_copy(
            src_ref=tiles.at[a, s], dst_ref=below.at[s],
            send_sem=below_send.at[s], recv_sem=below_recv.at[s],
            device_id=away(-1, 0), device_id_type=MESH,
        )

    def ships(s):
        return (lax.rem(target_of(s) + 1, rows) == my_row) & (target_of(s) + 1 < count)

    start_loads(local_cols - 1)
    partners = [away(0, o) for o in range(1, cols)] + [away(o, 0) for o in range(1, rows)]
    partners += [away(1, 1), away(-1, -1)]
    barrier = pltpu.get_barrier_semaphore()
    for partner in partners:
        pl.semaphore_signal(barrier, inc=1, device_id=partner, device_id_type=MESH)
    pl.semaphore_wait(barrier, len(partners))
    for s in reversed(range(local_cols - 1)):
        start_loads(s)

    for s in reversed(range(local_cols)):
        @pl.when(ships(s))
        def _():
            a = (target_of(s) + 1) // rows
            settle_in_place(a, s)
            below_copy(a, s).start()

    for s in range(local_cols):
        @pl.when(owns(s))
        def _():
            total[s] = target_ref[s, 0].T

        @pl.when(jnp.logical_not(owns(s)))
        def _():
            total[s] = jnp.zeros((rhs, width), jnp.float32)

    def prepare(s):
        k = target_of(s)
        settle_in_place(k // rows, s)
        invert(tiles.at[k // rows, s], inverse)
        size = min(128, width)

        def store(at, first, value):
            high, low = split(value)
            weights[s, first, pl.ds(at, size), :] = high
            weights[s, first + 1, pl.ds(at, size), :] = low

        def keep(p, carry):
            at = pl.multiple_of(p * size, size)
            store(at, 0, inverse[pl.ds(at, size), :])
            return carry

        lax.fori_loop(0, width // size, keep, 0)

        @pl.when(k + 1 < count)
        def _():
            below_copy(0, s).wait_recv()

            def correct(p, carry):
                at = pl.multiple_of(p * size, size)
                store(at, 2, split_product(below[s, pl.ds(at, size), :], weights[s, 0], weights[s, 1]))
                return carry

            lax.fori_loop(0, width // size, correct, 0)

    def accumulate(slot, s, where):
        total[s, where] = total[s, where] - split_product(
            solved_ref[slot, where], pairs[s, 0], pairs[s, 1]
        )

    def step(own_slot, j):
        slot = j // rows
        on_plane = my_row == lax.rem(j, rows)
        offset = lax.rem(lax.rem(j, cols) - my_col + cols, cols)
        owner = on_plane & (offset == 0)

        @pl.when(owner)
        def _():
            def solve(c, carry):
                here = span(c)
                for where, gap in reversed(list(enumerate(gaps))):
                    @pl.when(j + gap < count)
                    def _():
                        part_copy(own_slot, where, gap, c).wait_recv()
                        total[own_slot, here] = total[own_slot, here] + parts[own_slot, where, here]
                solved_ref[slot, here] = split_product(
                    total[own_slot, here], weights[own_slot, 0], weights[own_slot, 1]
                )

                @pl.when(j + 1 < count)
                def _():
                    chain_copy(slot, own_slot, c).wait_recv()
                    solved_ref[slot, here] = solved_ref[slot, here] - split_product(
                        chain[own_slot, here], weights[own_slot, 2], weights[own_slot, 3]
                    )

                @pl.when(j > 0)
                def _():
                    chain_copy(slot, (j - 1) // cols, c).start()
                for o in urgent:
                    plane_chunk(slot, o, c).start()
                return carry

            lax.fori_loop(0, CHUNKS, solve, 0)
            for o in calm:
                plane_whole(slot, o).start()

        @pl.when(on_plane)
        def _():
            for s in reversed(range(local_cols)):
                @pl.when(target_of(s) < j - 1)
                def _():
                    settle_pair(slot, s)

        is_urgent = on_plane & functools.reduce(
            jnp.logical_or, [offset == o for o in urgent], jnp.bool_(False)
        )

        @pl.when(is_urgent)
        def _():
            k = j - offset

            def follow(c, carry):
                plane_chunk(slot, 1, c).wait_recv()

                @pl.when(k >= 0)
                def _():
                    s = k // cols
                    accumulate(slot, s, span(c))
                    for where, gap in enumerate(gaps):
                        if gap in urgent:
                            @pl.when(offset == gap)
                            def _():
                                part_copy(s, where, gap, c).start()
                return carry

            lax.fori_loop(0, CHUNKS, follow, 0)

        @pl.when(on_plane & jnp.logical_not(is_urgent) & jnp.logical_not(owner))
        def _():
            plane_whole(slot, 1).wait_recv()

        @pl.when(on_plane)
        def _():
            for s in reversed(range(local_cols)):
                k = target_of(s)

                @pl.when((k < j - 1) & jnp.logical_not(is_urgent & (k == j - offset)))
                def _():
                    accumulate(slot, s, pl.ds(0, rhs))
                    for where, gap in enumerate(gaps):
                        if gap not in urgent:
                            @pl.when(k == j - gap)
                            def _():
                                for c in range(CHUNKS):
                                    part_copy(s, where, gap, c).start()

    def half(h, carry):
        own_slot = local_cols - 1 - h

        @pl.when(owns(own_slot))
        def _():
            prepare(own_slot)

        def one(o, inner):
            step(own_slot, (own_slot + 1) * cols - 1 - o)
            return inner

        return lax.fori_loop(0, cols, one, carry)

    lax.fori_loop(0, local_cols, half, 0)

    for s in reversed(range(local_cols)):
        @pl.when(ships(s))
        def _():
            below_copy(0, s).wait_send()

    def drain(i, carry):
        j = count - 1 - i
        slot = j // rows
        on_plane = my_row == lax.rem(j, rows)

        @pl.when(on_plane & (my_col == lax.rem(j, cols)))
        def _():
            def sent(c, inner):
                @pl.when(j > 0)
                def _():
                    chain_copy(slot, 0, c).wait_send()
                for o in urgent:
                    plane_chunk(slot, o, c).wait_send()
                return inner

            lax.fori_loop(0, CHUNKS, sent, 0)
            for o in calm:
                plane_whole(slot, o).wait_send()

        @pl.when(on_plane)
        def _():
            for s in range(local_cols):
                for where, gap in enumerate(gaps):
                    @pl.when(target_of(s) == j - gap)
                    def _():
                        for c in range(CHUNKS):
                            part_copy(s, where, gap, c).wait_send()
        return carry

    lax.fori_loop(0, count, drain, 0)


def sweep(rows, cols, wide, narrow, flags, target):
    local_rows, local_cols, width = wide.shape[0], wide.shape[2], wide.shape[4]
    rhs = target.shape[3]
    vmem = pl.BlockSpec(memory_space=pltpu.VMEM)
    hbm = pl.BlockSpec(memory_space=pl.ANY)
    dma = pltpu.SemaphoreType.DMA
    gaps = rows - 1
    return pl.pallas_call(
        functools.partial(sweep_kernel, rows, cols),
        out_shape=jax.ShapeDtypeStruct((local_rows, rhs, width), jnp.float32),
        in_specs=[hbm, hbm, pl.BlockSpec(memory_space=pltpu.SMEM), vmem],
        out_specs=vmem,
        scratch_shapes=[
            pltpu.VMEM((local_rows, local_cols, width, width), jnp.float32),
            pltpu.VMEM((local_rows, local_cols, width, width), jnp.bfloat16),
            pltpu.VMEM((local_cols, rhs, width), jnp.float32),
            pltpu.VMEM((local_cols, rhs, width), jnp.float32),
            pltpu.VMEM((local_cols, gaps, rhs, width), jnp.float32),
            pltpu.VMEM((local_cols, width, width), jnp.float32),
            pltpu.VMEM((width, width), jnp.float32),
            pltpu.VMEM((local_cols, 4, width, width), jnp.bfloat16),
            pltpu.VMEM((local_cols, 2, width, width), jnp.bfloat16),
            dma((local_rows, local_cols, 2)),
            dma((local_rows, CHUNKS)),
            dma((local_cols, CHUNKS)),
            dma((local_rows, cols, CHUNKS)),
            dma((local_rows, CHUNKS)),
            dma((local_cols, CHUNKS)),
            dma((local_cols, gaps, CHUNKS)),
            dma((local_cols,)),
            dma((local_cols,)),
        ],
        compiler_params=pltpu.CompilerParams(
            collective_id=0, has_side_effects=True, vmem_limit_bytes=VMEM_LIMIT
        ),
    )(wide, narrow, flags, target)


def finish_kernel(rows, cols, place_ref, solved_ref, x_ref, rhs_ref, grad_ref, left, right):
    a, s = pl.program_id(0), pl.program_id(1)
    local_cols, width = x_ref.shape[0], x_ref.shape[2]

    @pl.when((a == 0) & (s == 0))
    def _():
        for t in range(local_cols):
            high, low = split(x_ref[t, 0])
            right[t] = jnp.concatenate([high, high, low], axis=1)

    @pl.when(s == 0)
    def _():
        value = solved_ref[a].T
        rhs_ref[0, 0] = value
        high, low = split(-value)
        left[...] = jnp.concatenate([high, low, high], axis=1)

    i = a * rows + place_ref[0]
    k = s * cols + place_ref[1]

    def outer():
        return lax.dot_general(
            left[...], right[s], (((1,), (1,)), ((), ())), preferred_element_type=jnp.float32
        )

    @pl.when(i > k)
    def _():
        grad_ref[0, 0, 0, 0] = outer()

    @pl.when(i == k)
    def _():
        row = lax.broadcasted_iota(jnp.int32, (width, width), 0)
        col = lax.broadcasted_iota(jnp.int32, (width, width), 1)
        grad_ref[0, 0, 0, 0] = jnp.where(row >= col, outer(), 0.0)

    @pl.when(i < k)
    def _():
        grad_ref[0, 0, 0, 0] = jnp.zeros((width, width), jnp.float32)


def finish(rows, cols, place, solved, x):
    local_rows, rhs, width = solved.shape
    local_cols = x.shape[0]
    vmem = pl.BlockSpec(memory_space=pltpu.VMEM)
    return pl.pallas_call(
        functools.partial(finish_kernel, rows, cols),
        grid=(local_rows, local_cols),
        out_shape=(
            jax.ShapeDtypeStruct((local_rows, 1, width, rhs), jnp.float32),
            jax.ShapeDtypeStruct((local_rows, 1, local_cols, 1, width, width), jnp.float32),
        ),
        in_specs=[pl.BlockSpec(memory_space=pltpu.SMEM), vmem, vmem],
        out_specs=(
            pl.BlockSpec((1, 1, width, rhs), lambda a, s: (a, 0, 0, 0)),
            pl.BlockSpec((1, 1, 1, 1, width, width), lambda a, s: (a, 0, s, 0, 0, 0)),
        ),
        scratch_shapes=[
            pltpu.VMEM((width, 3 * rhs), jnp.bfloat16),
            pltpu.VMEM((local_cols, width, 3 * rhs), jnp.bfloat16),
        ],
    )(place, solved, x)


def body(factor_wide, factor_narrow, flags, forward_solution, solution_grad):
    rows, cols = lax.axis_size("row"), lax.axis_size("col")
    place = jnp.stack([lax.axis_index("row"), lax.axis_index("col")]).astype(jnp.int32)
    solved = sweep(rows, cols, factor_wide, factor_narrow, flags, solution_grad)
    return finish(rows, cols, place, solved, forward_solution)


def solution(mesh):
    placed = (
        P(None, "row", None, "col", None, None),
        P(None, "row", None, "col", None, None),
        P(None, "row", None, "col"),
        P(None, "col", None, None),
        P(None, "col", None, None),
    )
    return jax.shard_map(
        body,
        mesh=mesh,
        in_specs=placed,
        out_specs=(P(None, "row", None, None), P(None, "row", None, "col", None, None)),
        check_vma=False,
    )
```
